32 devices in a mesh: scen: 4 (over x, core), var: 8 (over z, y).
Axes of the slice: x: 2, y: 2, z: 4, core: 2. Of those that a mesh axis runs over, the one named last changes fastest.
Arguments:
- start_point: float32 [512, 65536], P('scen', 'var'), may hold values from -1 to 1
- multipliers: float32 [512, 65536], P('scen', 'var'), may hold values from -3 to 3
- cost: bfloat16 [512, 65536], P('scen', 'var'), may hold values from -6 to 6
- curvature: bfloat16 [512, 65536], P('scen', 'var'), may hold values from 0.5 to 2
- recourse_rhs: float32 [512, 512], P('scen'), may hold values from -12 to 12
- technology: bfloat16 [512, 65536], P(None, 'var'), may hold values from -0.0234375 to 0.0234375
- scenario_weight: float32 [512], P('scen'), may hold values from 1 to 30
- previous_mean: float32 [4, 65536], P(None, 'var'), may hold values from -1 to 1
- active: int32 [512, 512], P('scen', 'var'), may hold values 0 or 1
Outputs:
- iterate: float32 [512, 65536], P('scen', 'var')
- new_multipliers: float32 [512, 65536], P('scen', 'var')
- bundle_mean: float32 [4, 65536], P(None, 'var')
- primal_norm: float32 [], replicated
- dual_norm: float32 [], replicated
The draws below stay inside these ranges and needn't reach their ends.
All inputs are finite; a program needn't handle non-finite values. No bound on the sum of `active` on one device may be relied on, other than what follows from the above.
Results may differ from the reference program's by a relative error of at most 0.0007.
Values sent between devices are 32-bit elements; how exact they have to be, the bound alone decides.
A program may use at most 64 MiB of HBM per device.

```python
import math
import jax
import jax.numpy as jnp
from jax import lax

V = 65536
M = 512
BLK = 128
G = 4
STEPS = 8
SCENARIOS = 512


def rising_box(key, count):
    column = jnp.arange(V, dtype=jnp.float32)
    amplitude = (1.0 + 2.0 * column / (V - 1)) / 3.0
    first = jax.random.fold_in(jax.random.fold_in(key, 17), 0)
    values = jax.random.uniform(first, (count, V), jnp.float32, -1.0, 1.0)
    return (values * amplitude[None, :]).astype(jnp.float32)


def draw_start_point(key, part):
    return rising_box(jax.random.fold_in(key, 3), SCENARIOS)


def draw_previous_mean(key, part):
    return rising_box(jax.random.fold_in(key, 5), G)


def draw_scenario_weight(key, part):
    index = jnp.arange(SCENARIOS, dtype=jnp.float32)
    rising = 1.0 + 2.0 * index / (SCENARIOS - 1)
    noise_key = jax.random.fold_in(key, 7)
    base = jnp.exp(jax.random.uniform(noise_key, (SCENARIOS,), jnp.float32, 0.0, 2.302585))
    return jnp.clip(base * rising, 1.0, 30.0).astype(jnp.float32)


def with_ends(drawn, rng, least, high):
    longest = drawn.shape.index(max(drawn.shape))
    spots = []
    for shift in (0, 1):
        where = [jax.random.randint(jax.random.fold_in(rng, axis), (), 0, length) for axis, length in enumerate(drawn.shape)]
        where[longest] = (where[longest] + shift) % drawn.shape[longest]
        spots.append(tuple(where))
    return drawn.at[spots[0]].set(least).at[spots[1]].set(high)


def block_levels(rng, shape, shards, low, top_value):
    def one(position, shards_of):
        draws = jax.random.uniform(jax.random.fold_in(jax.random.fold_in(rng, 6), position), (shards_of,), jnp.float32, low / len(shards), top_value / len(shards))
        return jnp.repeat(jnp.exp(draws), shape[position] // shards_of).reshape((-1,) + (1,) * (len(shape) - position - 1))

    loudness = one(*shards[0])
    for cut in shards[1:]:
        loudness = loudness * one(*cut)
    return loudness


def normal_values(rng, dims, width, reach, shards=(), held_as=jnp.bfloat16):
    array = width * jax.random.normal(rng, dims, jnp.float32)
    if shards:
        array = array * block_levels(rng, dims, shards, -0.22, 0.18)
    return jnp.clip(array, -reach, reach).astype(held_as)


def setup_inputs(seed: int = 0) -> dict:
    key_of = jax.random.split(jax.random.key(seed), 10)
    return {
        "start_point": draw_start_point(jax.random.fold_in(key_of[9], 71), 0),
        "multipliers": normal_values(key_of[1], (SCENARIOS, V), 0.5, 3.0, ((0, 4), (1, 8)), jnp.float32),
        "cost": normal_values(key_of[2], (SCENARIOS, V), 1.0, 6.0, ((0, 4), (1, 8))),
        "curvature": jnp.clip(jnp.exp(math.log(2.0) - 1.3862944 * jax.random.uniform(key_of[3], (SCENARIOS, V), jnp.float32) ** block_levels(key_of[3], (SCENARIOS, V), ((0, 4), (1, 8)), -0.2, 0.2)), 0.5, 2.0).astype(jnp.bfloat16),
        "recourse_rhs": normal_values(key_of[4], (SCENARIOS, M), 3.0, 12.0, ((0, 4),), jnp.float32),
        "technology": normal_values(key_of[5], (M, V), V ** -0.5, 0.0234375, ((1, 8),)),
        "scenario_weight": draw_scenario_weight(jax.random.fold_in(key_of[9], 71), 0),
        "previous_mean": draw_previous_mean(jax.random.fold_in(key_of[9], 71), 0),
        "active": with_ends((jax.random.randint(key_of[8], (SCENARIOS, V // BLK), 0, 4) < 3).astype(jnp.int32), jax.random.fold_in(key_of[8], 1), 0, 1),
    }


highest = lax.Precision.HIGHEST
penalty = 1.0
recourse_scale = 4.0
stride = 0.2
epsilon = 1e-06

def reference(start_point, multipliers, cost, curvature, recourse_rhs, technology, scenario_weight, previous_mean, active):
    node_of = jnp.arange(SCENARIOS, dtype=jnp.int32) // (SCENARIOS // G)
    member = (node_of[:, None] == jnp.arange(G, dtype=jnp.int32)[None, :]).astype(jnp.float32)
    anchor = jnp.dot(member, previous_mean, precision=highest, preferred_element_type=jnp.float32)
    linear = cost.astype(jnp.float32) + multipliers - penalty * anchor
    diagonal = curvature.astype(jnp.float32) + penalty
    active_mask = jnp.repeat(active > 0, BLK, axis=1)
    iterate = start_point
    for sweep in range(STEPS):
        rounded = iterate.astype(jnp.bfloat16)
        image = lax.dot_general(rounded, technology, (((1,), (1,)), ((), ())), preferred_element_type=jnp.float32)
        shortfall = (image - recourse_rhs).astype(jnp.bfloat16)
        pullback = jnp.dot(shortfall, technology, preferred_element_type=jnp.float32)
        stepped = jnp.clip(iterate - stride * (diagonal * iterate + linear + recourse_scale * pullback), -1.0, 1.0)
        iterate = jnp.where(active_mask, stepped, iterate)
    weighted = scenario_weight[:, None] * iterate
    totals = lax.dot_general(member, weighted, (((0,), (0,)), ((), ())), precision=highest, preferred_element_type=jnp.float32)
    bundle_mass = lax.optimization_barrier(jnp.sum(member * scenario_weight[:, None], axis=0))
    bundle_mean = totals / bundle_mass[:, None]
    centred = iterate - jnp.dot(member, bundle_mean, precision=highest, preferred_element_type=jnp.float32)
    spread = jnp.sum(scenario_weight[:, None] * centred * centred)
    drift_sum = jnp.sum(bundle_mass[:, None] * (bundle_mean - previous_mean) ** 2)
    normaliser = jnp.sum(bundle_mass) * V
    primal_norm = jnp.sqrt(spread / normaliser + epsilon)
    dual_norm = penalty * jnp.sqrt(drift_sum / normaliser + epsilon)
    factor = penalty * jnp.sqrt(primal_norm / dual_norm)
    new_multipliers = multipliers + factor * centred
    return (iterate, new_multipliers, bundle_mean, primal_norm, dual_norm)
```

```python
import functools

import jax
import jax.numpy as jnp
from jax import lax
from jax.experimental import pallas as pl
from jax.experimental.pallas import tpu as pltpu
from jax.sharding import PartitionSpec as P

BLK = 128
STEPS = 8
LANES = 128

penalty = 1.0
recourse_scale = 4.0
stride = 0.2
epsilon = 1e-06


def kernel(
    n, count, nodes, pieces, sets,
    start_hbm, mult_hbm, cost_hbm, curv_hbm, rhs_ref, tech_hbm, weight_ref, prev_ref, active_ref,
    iterate_hbm, new_mult_hbm, mean_ref, norms_ref,
    tech, it, mult, cost, curv, keep, push, gate, part, landed, full, short, own, totals, scal_var, scal_scen,
    load_sem, store_sem, rs_send, rs_recv, ag_send, ag_recv, t_send, t_recv, v_send, v_recv, s_send, s_recv,
):
    me = lax.axis_index("var")
    pos = lax.axis_index("scen")
    per_node = count // nodes
    my_node = pos // per_node
    rows, cols = it.shape
    width = cols // pieces
    height = rows // sets

    def load(which, src, dst, piece):
        where = (slice(None), pl.ds(piece * width, width))
        return pltpu.make_async_copy(src.at[where], dst.at[where], load_sem.at[which, piece])

    loads = ((start_hbm, it), (tech_hbm, tech), (mult_hbm, mult), (cost_hbm, cost), (curv_hbm, curv))
    for early in ((0, 1), (2, 3, 4)):
        for piece in range(pieces):
            for which in early:
                load(which, *loads[which], piece).start()

    barrier = pltpu.get_barrier_semaphore()
    for k in range(1, n):
        pl.semaphore_signal(barrier, inc=1, device_id={"var": lax.rem(me + k, n)})
    for k in range(1, count):
        pl.semaphore_signal(barrier, inc=1, device_id={"scen": lax.rem(pos + k, count)})
    pl.semaphore_wait(barrier, n + count - 2)

    def scatter(g, k):
        to = lax.rem(me + k, n)
        return pltpu.make_async_remote_copy(
            src_ref=part.at[g, to], dst_ref=landed.at[g, k - 1],
            send_sem=rs_send.at[g, k - 1], recv_sem=rs_recv.at[g, k - 1], device_id={"var": to},
        )

    def gather(g, k):
        return pltpu.make_async_remote_copy(
            src_ref=full.at[g, me], dst_ref=full.at[g, me],
            send_sem=ag_send.at[g, k - 1], recv_sem=ag_recv.at[g, k - 1],
            device_id={"var": lax.rem(me + k, n)},
        )

    def pick_row(ref):
        row = ref[0:1, :]
        for node in range(1, nodes):
            row = jnp.where(my_node == node, ref[node : node + 1, :], row)
        own[...] = row

    def image_of(g, where):
        rounded = it[pl.ds(g * height, height), where].astype(jnp.bfloat16)
        found = lax.dot_general(
            rounded, tech[:, where], (((1,), (1,)), ((), ())), preferred_element_type=jnp.float32
        )
        return found.reshape(part.shape[1:])

    def send_parts(g):
        for k in range(1, n):
            scatter(g, k).start()

    for piece in range(pieces):
        where = pl.ds(piece * width, width)
        for which in (0, 1):
            load(which, *loads[which], piece).wait()
        for g in range(sets):
            found = image_of(g, where)
            part[g] = found if piece == 0 else part[g] + found
    for g in range(sets):
        send_parts(g)

    pick_row(prev_ref)
    for piece in range(pieces):
        for which in (2, 3, 4):
            load(which, *loads[which], piece).wait()
        for block in range(piece * (width // BLK), (piece + 1) * (width // BLK)):
            where = pl.ds(block * BLK, BLK)
            on = jnp.broadcast_to((active_ref[:, block : block + 1] > 0).astype(jnp.float32), (rows, BLK))
            linear = cost[:, where].astype(jnp.float32) + mult[:, where] - penalty * own[:, where]
            diagonal = curv[:, where].astype(jnp.float32) + penalty
            keep[:, where] = 1.0 - stride * diagonal * on
            push[:, where] = stride * linear * on
            gate[:, where] = stride * recourse_scale * on

    def reduce_parts():
        for g in range(sets):
            for k in range(1, n):
                scatter(g, k).wait_recv()
            found = part[g, me]
            for k in range(1, n):
                found = found + landed[g, k - 1]
            full[g, me] = found
            for k in range(1, n):
                gather(g, k).start()
            for k in range(1, n):
                scatter(g, k).wait_send()

    def take_image(g):
        for k in range(1, n):
            gather(g, k).wait_recv()
        image = full[g].reshape(height, full.shape[-1])
        short[g] = (image - rhs_ref[pl.ds(g * height, height), :]).astype(jnp.bfloat16)
        for k in range(1, n):
            gather(g, k).wait_send()

    def move(g, where):
        mine = pl.ds(g * height, height)
        pullback = jnp.dot(short[g], tech[:, where], preferred_element_type=jnp.float32)
        stepped = keep[mine, where] * it[mine, where] - push[mine, where] - gate[mine, where] * pullback
        new = jnp.clip(stepped, -1.0, 1.0)
        it[mine, where] = new
        return new

    def sweep(step, carry):
        reduce_parts()
        for g in range(sets):
            take_image(g)
            part[g] = jnp.zeros(part.shape[1:], jnp.float32)

            def one(piece, carry):
                where = pl.ds(pl.multiple_of(piece * width, width), width)
                move(g, where)
                part[g] = part[g] + image_of(g, where)
                return carry

            lax.fori_loop(0, pieces, one, 0)
            send_parts(g)
        return carry

    lax.fori_loop(0, STEPS - 1, sweep, 0)

    reduce_parts()
    weights = weight_ref[...]
    for g in range(sets):
        take_image(g)

        def last(piece, carry):
            where = pl.ds(pl.multiple_of(piece * width, width), width)
            new = move(g, where)
            total = jnp.sum(weights[g * height : (g + 1) * height] * new, axis=0, keepdims=True)
            totals[pos, :, where] = total if g == 0 else totals[pos, :, where] + total
            return carry

        lax.fori_loop(0, pieces, last, 0)
    totals[pos, :, pl.ds(cols, LANES)] = jnp.broadcast_to(jnp.sum(weights, axis=0, keepdims=True), (1, LANES))

    def share(ref, spot, axis, size, sends, recvs, k):
        return pltpu.make_async_remote_copy(
            src_ref=ref.at[spot], dst_ref=ref.at[spot], send_sem=sends.at[k - 1], recv_sem=recvs.at[k - 1],
            device_id={axis: lax.rem(spot + k, size)},
        )

    def spread_out(*what):
        for k in range(1, what[3]):
            share(*what, k).start()

    def collect(*what):
        for k in range(1, what[3]):
            share(*what, k).wait()

    exchange_t = (totals, pos, "scen", count, t_send, t_recv)
    spread_out(*exchange_t)
    out_it = pltpu.make_async_copy(it, iterate_hbm, store_sem.at[pieces])
    out_it.start()
    collect(*exchange_t)

    def mass_of(node):
        found = totals[node * per_node, :, pl.ds(cols, 1)]
        for p in range(node * per_node + 1, (node + 1) * per_node):
            found = found + totals[p, :, pl.ds(cols, 1)]
        return found

    masses = [mass_of(node) for node in range(nodes)]
    all_mass = masses[0]
    for mass in masses[1:]:
        all_mass = all_mass + mass

    drift = jnp.zeros((1, 1), jnp.float32)
    for node in range(nodes):
        total = totals[node * per_node, :, pl.ds(0, cols)]
        for p in range(node * per_node + 1, (node + 1) * per_node):
            total = total + totals[p, :, pl.ds(0, cols)]
        mean = total / masses[node]
        mean_ref[node : node + 1, :] = mean
        gap = mean - prev_ref[node : node + 1, :]
        drift = drift + masses[node] * jnp.sum(gap * gap, axis=1, keepdims=True)

    pick_row(mean_ref)

    def apart(piece):
        where = pl.ds(pl.multiple_of(piece * width, width), width)
        return where, it[:, where] - own[:, where]

    def widen(piece, carry):
        where, centred = apart(piece)
        return carry + jnp.sum(weights * centred * centred, axis=0, keepdims=True)

    spread = lax.fori_loop(0, pieces, widen, jnp.zeros((1, width), jnp.float32))
    spread = jnp.sum(spread, axis=1, keepdims=True)

    first_row = lax.broadcasted_iota(jnp.int32, scal_var.shape[1:], 0) == 0
    scal_var[me] = jnp.where(first_row, spread, drift)
    exchange_v = (scal_var, me, "var", n, v_send, v_recv)
    spread_out(*exchange_v)
    collect(*exchange_v)
    both = scal_var[0]
    for p in range(1, n):
        both = both + scal_var[p]
    scal_scen[pos] = both
    exchange_s = (scal_scen, pos, "scen", count, s_send, s_recv)
    spread_out(*exchange_s)
    collect(*exchange_s)
    both = scal_scen[0]
    drift = both[1:2, 0:1]
    for p in range(1, count):
        both = both + scal_scen[p]
    spread = both[0:1, 0:1]
    normaliser = all_mass * float(n * cols)
    primal = jnp.sqrt(spread / normaliser + epsilon)
    dual = penalty * jnp.sqrt(drift / normaliser + epsilon)
    factor = penalty * jnp.sqrt(primal / dual)
    norms_ref[...] = jnp.where(first_row, primal, dual)

    def store(piece):
        where = pl.ds(piece * width, width)
        return pltpu.make_async_copy(mult.at[:, where], new_mult_hbm.at[:, where], store_sem.at[piece])

    for piece in range(pieces):
        where, centred = apart(piece)
        mult[:, where] = mult[:, where] + factor * centred
        store(piece).start()
    for piece in range(pieces):
        store(piece).wait()
    out_it.wait()


def solution(mesh):
    n, count = mesh.shape["var"], mesh.shape["scen"]

    def shards(start, multipliers, cost, curvature, rhs, technology, weight, previous, active):
        rows, cols = start.shape
        m = technology.shape[0]
        nodes = previous.shape[0]
        sets = 2 if rows % (16 * n) == 0 else 1
        chunk = rows // sets // n
        pieces = 8
        f32 = jnp.float32
        dma = pltpu.SemaphoreType.DMA
        anywhere = pl.BlockSpec(memory_space=pl.ANY)
        vmem = pl.BlockSpec(memory_space=pltpu.VMEM)
        iterate, new_multipliers, mean, norms = pl.pallas_call(
            functools.partial(kernel, n, count, nodes, pieces, sets),
            out_shape=(
                jax.ShapeDtypeStruct((rows, cols), f32),
                jax.ShapeDtypeStruct((rows, cols), f32),
                jax.ShapeDtypeStruct((nodes, cols), f32),
                jax.ShapeDtypeStruct((8, LANES), f32),
            ),
            in_specs=[anywhere] * 4 + [vmem, anywhere, vmem, vmem, vmem],
            out_specs=(anywhere, anywhere, vmem, vmem),
            scratch_shapes=[
                pltpu.VMEM((m, cols), jnp.bfloat16),
                pltpu.VMEM((rows, cols), f32),
                pltpu.VMEM((rows, cols), f32),
                pltpu.VMEM((rows, cols), jnp.bfloat16),
                pltpu.VMEM((rows, cols), jnp.bfloat16),
                pltpu.VMEM((rows, cols), f32),
                pltpu.VMEM((rows, cols), f32),
                pltpu.VMEM((rows, cols), f32),
                pltpu.VMEM((sets, n, chunk, m), f32),
                pltpu.VMEM((sets, n - 1, chunk, m), f32),
                pltpu.VMEM((sets, n, chunk, m), f32),
                pltpu.VMEM((sets, rows // sets, m), jnp.bfloat16),
                pltpu.VMEM((1, cols), f32),
                pltpu.VMEM((count, 1, cols + LANES), f32),
                pltpu.VMEM((n, 8, LANES), f32),
                pltpu.VMEM((count, 8, LANES), f32),
                dma((5, pieces)),
                dma((pieces + 1,)),
                dma((sets, n - 1)),
                dma((sets, n - 1)),
                dma((sets, n - 1)),
                dma((sets, n - 1)),
                dma((count - 1,)),
                dma((count - 1,)),
                dma((n - 1,)),
                dma((n - 1,)),
                dma((count - 1,)),
                dma((count - 1,)),
            ],
            compiler_params=pltpu.CompilerParams(
                collective_id=0, has_side_effects=True, vmem_limit_bytes=60 * 1024 * 1024
            ),
        )(start, multipliers, cost, curvature, rhs, technology, weight.reshape(rows, 1), previous, active)
        return iterate, new_multipliers, mean, norms[0, 0], norms[1, 0]

    both = P("scen", "var")
    return jax.shard_map(
        shards,
        mesh=mesh,
        in_specs=(both, both, both, both, P("scen", None), P(None, "var"), P("scen"), P(None, "var"), both),
        out_specs=(both, both, P(None, "var"), P(), P()),
        check_vma=False,
    )
```

```python
import functools

import jax
import jax.numpy as jnp
from jax import lax
from jax.experimental import pallas as pl
from jax.experimental.pallas import tpu as pltpu
from jax.sharding import PartitionSpec as P

BLK = 128
STEPS = 8
LANES = 128

penalty = 1.0
recourse_scale = 4.0
stride = 0.2
epsilon = 1e-06


def kernel(
    n, count, nodes, pieces, sets,
    start_hbm, mult_hbm, cost_hbm, curv_hbm, rhs_ref, tech_hbm, weight_ref, prev_ref, active_ref,
    iterate_hbm, new_mult_hbm, mean_ref, norms_ref,
    tech, it, mult, cost, curv, keep, push, gate, part, landed, full, short, own, totals, scal_var, scal_scen,
    load_sem, store_sem, rs_send, rs_recv, ag_send, ag_recv, t_send, t_recv, v_send, v_recv, s_send, s_recv,
):
    me = lax.axis_index("var")
    pos = lax.axis_index("scen")
    per_node = count // nodes
    my_node = pos // per_node
    rows, cols = it.shape
    width = cols // pieces
    height = rows // sets

    def load(which, src, dst, piece):
        where = (slice(None), pl.ds(piece * width, width))
        return pltpu.make_async_copy(src.at[where], dst.at[where], load_sem.at[which, piece])

    loads = ((start_hbm, it), (tech_hbm, tech), (mult_hbm, mult), (cost_hbm, cost), (curv_hbm, curv))
    for early in ((0, 1), (2, 3, 4)):
        for piece in range(pieces):
            for which in early:
                load(which, *loads[which], piece).start()

    barrier = pltpu.get_barrier_semaphore()
    for k in range(1, n):
        pl.semaphore_signal(barrier, inc=1, device_id={"var": lax.rem(me + k, n)})
    for k in range(1, count):
        pl.semaphore_signal(barrier, inc=1, device_id={"scen": lax.rem(pos + k, count)})
    pl.semaphore_wait(barrier, n + count - 2)

    def scatter(g, k):
        to = lax.rem(me + k, n)
        return pltpu.make_async_remote_copy(
            src_ref=part.at[g, to], dst_ref=landed.at[g, k - 1],
            send_sem=rs_send.at[g, k - 1], recv_sem=rs_recv.at[g, k - 1], device_id={"var": to},
        )

    def gather(g, k):
        return pltpu.make_async_remote_copy(
            src_ref=full.at[g, me], dst_ref=full.at[g, me],
            send_sem=ag_send.at[g, k - 1], recv_sem=ag_recv.at[g, k - 1],
            device_id={"var": lax.rem(me + k, n)},
        )

    def pick_row(ref):
        row = ref[0:1, :]
        for node in range(1, nodes):
            row = jnp.where(my_node == node, ref[node : node + 1, :], row)
        own[...] = row

    def image_of(g, where):
        rounded = it[pl.ds(g * height, height), where].astype(jnp.bfloat16)
        found = lax.dot_general(
            rounded, tech[:, where], (((1,), (1,)), ((), ())), preferred_element_type=jnp.float32
        )
        return found.reshape(part.shape[1:])

    def send_parts(g):
        for k in range(1, n):
            scatter(g, k).start()

    for piece in range(pieces):
        where = pl.ds(piece * width, width)
        for which in (0, 1):
            load(which, *loads[which], piece).wait()
        for g in range(sets):
            found = image_of(g, where)
            part[g] = found if piece == 0 else part[g] + found
    for g in range(sets):
        send_parts(g)

    active = jnp.transpose((active_ref[...] > 0).astype(jnp.float32))
    pick_row(prev_ref)
    for piece in range(pieces):
        for which in (2, 3, 4):
            load(which, *loads[which], piece).wait()
        for block in range(piece * (width // BLK), (piece + 1) * (width // BLK)):
            where = pl.ds(block * BLK, BLK)
            on = jnp.broadcast_to(active[:, block : block + 1], (rows, BLK))
            linear = cost[:, where].astype(jnp.float32) + mult[:, where] - penalty * own[:, where]
            diagonal = curv[:, where].astype(jnp.float32) + penalty
            keep[:, where] = 1.0 - stride * diagonal * on
            push[:, where] = stride * linear * on
            gate[:, where] = stride * recourse_scale * on

    def reduce_parts():
        for g in range(sets):
            for k in range(1, n):
                scatter(g, k).wait_recv()
            found = part[g, me]
            for k in range(1, n):
                found = found + landed[g, k - 1]
            full[g, me] = found
            for k in range(1, n):
                gather(g, k).start()
            for k in range(1, n):
                scatter(g, k).wait_send()

    def take_image(g):
        for k in range(1, n):
            gather(g, k).wait_recv()
        image = full[g].reshape(height, full.shape[-1])
        short[g] = (image - rhs_ref[pl.ds(g * height, height), :]).astype(jnp.bfloat16)
        for k in range(1, n):
            gather(g, k).wait_send()

    def move(g, where):
        mine = pl.ds(g * height, height)
        pullback = jnp.dot(short[g], tech[:, where], preferred_element_type=jnp.float32)
        stepped = keep[mine, where] * it[mine, where] - push[mine, where] - gate[mine, where] * pullback
        new = jnp.clip(stepped, -1.0, 1.0)
        it[mine, where] = new
        return new

    def sweep(step, carry):
        reduce_parts()
        for g in range(sets):
            take_image(g)
            part[g] = jnp.zeros(part.shape[1:], jnp.float32)

            def one(piece, carry):
                where = pl.ds(pl.multiple_of(piece * width, width), width)
                move(g, where)
                part[g] = part[g] + image_of(g, where)
                return carry

            lax.fori_loop(0, pieces, one, 0)
            send_parts(g)
        return carry

    lax.fori_loop(0, STEPS - 1, sweep, 0)

    reduce_parts()
    weights = jnp.transpose(jnp.broadcast_to(weight_ref[...], (LANES, rows)))[:, 0:1]
    for g in range(sets):
        take_image(g)

        def last(piece, carry):
            where = pl.ds(pl.multiple_of(piece * width, width), width)
            new = move(g, where)
            total = jnp.sum(weights[g * height : (g + 1) * height] * new, axis=0, keepdims=True)
            totals[pos, :, where] = total if g == 0 else totals[pos, :, where] + total
            return carry

        lax.fori_loop(0, pieces, last, 0)
    totals[pos, :, pl.ds(cols, LANES)] = jnp.broadcast_to(jnp.sum(weights, axis=0, keepdims=True), (1, LANES))

    def share(ref, spot, axis, size, sends, recvs, k):
        return pltpu.make_async_remote_copy(
            src_ref=ref.at[spot], dst_ref=ref.at[spot], send_sem=sends.at[k - 1], recv_sem=recvs.at[k - 1],
            device_id={axis: lax.rem(spot + k, size)},
        )

    def spread_out(*what):
        for k in range(1, what[3]):
            share(*what, k).start()

    def collect(*what):
        for k in range(1, what[3]):
            share(*what, k).wait()

    exchange_t = (totals, pos, "scen", count, t_send, t_recv)
    spread_out(*exchange_t)
    out_it = pltpu.make_async_copy(it, iterate_hbm, store_sem.at[pieces])
    out_it.start()
    collect(*exchange_t)

    def mass_of(node):
        found = totals[node * per_node, :, pl.ds(cols, 1)]
        for p in range(node * per_node + 1, (node + 1) * per_node):
            found = found + totals[p, :, pl.ds(cols, 1)]
        return found

    masses = [mass_of(node) for node in range(nodes)]
    all_mass = masses[0]
    for mass in masses[1:]:
        all_mass = all_mass + mass

    drift = jnp.zeros((1, 1), jnp.float32)
    for node in range(nodes):
        total = totals[node * per_node, :, pl.ds(0, cols)]
        for p in range(node * per_node + 1, (node + 1) * per_node):
            total = total + totals[p, :, pl.ds(0, cols)]
        mean = total / masses[node]
        mean_ref[node : node + 1, :] = mean
        gap = mean - prev_ref[node : node + 1, :]
        drift = drift + masses[node] * jnp.sum(gap * gap, axis=1, keepdims=True)

    pick_row(mean_ref)

    def apart(piece):
        where = pl.ds(pl.multiple_of(piece * width, width), width)
        return where, it[:, where] - own[:, where]

    def widen(piece, carry):
        where, centred = apart(piece)
        return carry + jnp.sum(weights * centred * centred, axis=0, keepdims=True)

    spread = lax.fori_loop(0, pieces, widen, jnp.zeros((1, width), jnp.float32))
    spread = jnp.sum(spread, axis=1, keepdims=True)

    first_row = lax.broadcasted_iota(jnp.int32, scal_var.shape[1:], 0) == 0
    scal_var[me] = jnp.where(first_row, spread, drift)
    exchange_v = (scal_var, me, "var", n, v_send, v_recv)
    spread_out(*exchange_v)
    collect(*exchange_v)
    both = scal_var[0]
    for p in range(1, n):
        both = both + scal_var[p]
    scal_scen[pos] = both
    exchange_s = (scal_scen, pos, "scen", count, s_send, s_recv)
    spread_out(*exchange_s)
    collect(*exchange_s)
    both = scal_scen[0]
    drift = both[1:2, 0:1]
    for p in range(1, count):
        both = both + scal_scen[p]
    spread = both[0:1, 0:1]
    normaliser = all_mass * float(n * cols)
    primal = jnp.sqrt(spread / normaliser + epsilon)
    dual = penalty * jnp.sqrt(drift / normaliser + epsilon)
    factor = penalty * jnp.sqrt(primal / dual)
    norms_ref[...] = jnp.where(first_row, primal, dual)

    def store(piece):
        where = pl.ds(piece * width, width)
        return pltpu.make_async_copy(mult.at[:, where], new_mult_hbm.at[:, where], store_sem.at[piece])

    for piece in range(pieces):
        where, centred = apart(piece)
        mult[:, where] = mult[:, where] + factor * centred
        store(piece).start()
    for piece in range(pieces):
        store(piece).wait()
    out_it.wait()


def solution(mesh):
    n, count = mesh.shape["var"], mesh.shape["scen"]

    def shards(start, multipliers, cost, curvature, rhs, technology, weight, previous, active):
        rows, cols = start.shape
        m = technology.shape[0]
        nodes = previous.shape[0]
        sets = 2 if rows % (16 * n) == 0 else 1
        chunk = rows // sets // n
        pieces = 8
        f32 = jnp.float32
        dma = pltpu.SemaphoreType.DMA
        anywhere = pl.BlockSpec(memory_space=pl.ANY)
        vmem = pl.BlockSpec(memory_space=pltpu.VMEM)
        iterate, new_multipliers, mean, norms = pl.pallas_call(
            functools.partial(kernel, n, count, nodes, pieces, sets),
            out_shape=(
                jax.ShapeDtypeStruct((rows, cols), f32),
                jax.ShapeDtypeStruct((rows, cols), f32),
                jax.ShapeDtypeStruct((nodes, cols), f32),
                jax.ShapeDtypeStruct((8, LANES), f32),
            ),
            in_specs=[anywhere] * 4 + [vmem, anywhere, vmem, vmem, vmem],
            out_specs=(anywhere, anywhere, vmem, vmem),
            scratch_shapes=[
                pltpu.VMEM((m, cols), jnp.bfloat16),
                pltpu.VMEM((rows, cols), f32),
                pltpu.VMEM((rows, cols), f32),
                pltpu.VMEM((rows, cols), jnp.bfloat16),
                pltpu.VMEM((rows, cols), jnp.bfloat16),
                pltpu.VMEM((rows, cols), f32),
                pltpu.VMEM((rows, cols), f32),
                pltpu.VMEM((rows, cols), f32),
                pltpu.VMEM((sets, n, chunk, m), f32),
                pltpu.VMEM((sets, n - 1, chunk, m), f32),
                pltpu.VMEM((sets, n, chunk, m), f32),
                pltpu.VMEM((sets, rows // sets, m), jnp.bfloat16),
                pltpu.VMEM((1, cols), f32),
                pltpu.VMEM((count, 1, cols + LANES), f32),
                pltpu.VMEM((n, 8, LANES), f32),
                pltpu.VMEM((count, 8, LANES), f32),
                dma((5, pieces)),
                dma((pieces + 1,)),
                dma((sets, n - 1)),
                dma((sets, n - 1)),
                dma((sets, n - 1)),
                dma((sets, n - 1)),
                dma((count - 1,)),
                dma((count - 1,)),
                dma((n - 1,)),
                dma((n - 1,)),
                dma((count - 1,)),
                dma((count - 1,)),
            ],
            compiler_params=pltpu.CompilerParams(
                collective_id=0, has_side_effects=True, vmem_limit_bytes=60 * 1024 * 1024
            ),
        )(start, multipliers, cost, curvature, rhs, technology, weight.reshape(1, rows), previous, active.T)
        return iterate, new_multipliers, mean, norms[0, 0], norms[1, 0]

    both = P("scen", "var")
    return jax.shard_map(
        shards,
        mesh=mesh,
        in_specs=(both, both, both, both, P("scen", None), P(None, "var"), P("scen"), P(None, "var"), both),
        out_specs=(both, both, P(None, "var"), P(), P()),
        check_vma=False,
    )
```
